32 devices in a mesh: tm: 4 (over y, x), space: 8 (over z, core).
Axes of the slice: x: 2, y: 2, z: 4, core: 2. Of those that a mesh axis runs over, the one named last changes fastest.
Arguments:
- thermal_field: float32 [128, 49152], P(('tm', 'space')), may hold values from 245 to 255
- seasonal_bucket: int32 [128], replicated, may hold values from 0 to 45, as said below
- season_of_record: int32 [128], replicated, may hold values from 0 to 7
Outputs:
- anomaly: float32 [128, 49152], P(('tm', 'space'))
The draws below stay inside these ranges and needn't reach their ends.
Inputs may be any that keep to these rules, and one draw needn't show every extreme that they name: `seasonal_bucket`: every group holds at least one day whose year is below 6.
All inputs are finite; a program needn't handle non-finite values.
Results may differ from the reference program's by a relative error of at most 0.0003.
Values sent between devices are 32-bit elements; how exact they have to be, the bound alone decides.
A program may use at most 64 MiB of HBM per device.

```python
import jax
import jax.numpy as jnp
from jax import lax

GROUPS = 46
YEARS = 8
BASE_YEARS = 6
TIME_STEPS = 128
MESH_POINTS = 49152


def calendar(key):
    ordering = jax.random.permutation(jax.random.fold_in(key, 11), TIME_STEPS)
    chosen_records = ordering[:GROUPS]
    random_group = jax.random.randint(jax.random.fold_in(key, 12), (TIME_STEPS,), 0, GROUPS)
    random_year = jax.random.randint(jax.random.fold_in(key, 13), (TIME_STEPS,), 0, YEARS)
    base_year = jax.random.randint(jax.random.fold_in(key, 14), (GROUPS,), 0, BASE_YEARS)
    groups = random_group.at[chosen_records].set(jnp.arange(GROUPS, dtype=jnp.int32))
    years = random_year.at[chosen_records].set(base_year)
    return (groups.astype(jnp.int32), years.astype(jnp.int32))


def draw_seasonal_bucket(key, part):
    return calendar(key)[0]


def draw_season_of_record(key, part):
    return calendar(key)[1]


def steps_of(rng, shape, pieces, least, high):
    def one(dim, blocks):
        steps = jax.random.uniform(jax.random.fold_in(jax.random.fold_in(rng, 6), dim), (blocks,), jnp.float32, least / len(pieces), high / len(pieces))
        return jnp.repeat(jnp.exp(steps), shape[dim] // blocks).reshape((-1,) + (1,) * (len(shape) - dim - 1))

    level = one(*pieces[0])
    for cut in pieces[1:]:
        level = level * one(*cut)
    return level


def setup_inputs(seed: int = 0) -> dict:
    splits = jax.random.split(jax.random.key(seed), 4)
    return {
        "thermal_field": jnp.clip(245.0 + 10.0 * jax.random.uniform(splits[0], (TIME_STEPS, MESH_POINTS), jnp.float32) ** steps_of(splits[0], (TIME_STEPS, MESH_POINTS), ((0, 32),), -0.2, 0.2), 245.0, 255.0),
        "seasonal_bucket": draw_seasonal_bucket(jax.random.fold_in(splits[3], 71), 0),
        "season_of_record": draw_season_of_record(jax.random.fold_in(splits[3], 71), 0),
    }


def reference(thermal_field, seasonal_bucket, season_of_record):
    group_ids = jnp.arange(GROUPS, dtype=jnp.int32)
    member = (seasonal_bucket[None, :] == group_ids[:, None]).astype(jnp.float32)
    reference_seasons = member * (season_of_record < BASE_YEARS).astype(jnp.float32)[None, :]
    counts = jnp.sum(reference_seasons, axis=1)
    bucket_aggregates = jnp.dot(reference_seasons, thermal_field, precision=lax.Precision.HIGHEST, preferred_element_type=jnp.float32)
    climate = bucket_aggregates / counts[:, None]
    chosen_records = jnp.dot(member.T, climate, precision=lax.Precision.HIGHEST, preferred_element_type=jnp.float32)
    return thermal_field - chosen_records
```

```python
import functools

import jax
import jax.numpy as jnp
from jax import lax
from jax.experimental import pallas as pl
from jax.experimental.pallas import tpu as pltpu
from jax.sharding import PartitionSpec as P

GROUPS = 46
BASE_YEARS = 6
PLANES = 4
UNIT = 128
RAW = 12
SIZES = (2, 3, 3, 3, 3, 3, 3, 3, 3, 3, 3, 2, 2)
LAG = 2
RELAYS = 3
SPREAD = 3
SOLVE = 6
MESH = pl.DeviceIdType.MESH


def exact_dot(mask, x):
    high = x.astype(jnp.bfloat16)
    rest = x - high.astype(jnp.float32)
    middle = rest.astype(jnp.bfloat16)
    low = (rest - middle.astype(jnp.float32)).astype(jnp.bfloat16)
    total = jnp.dot(mask, low, preferred_element_type=jnp.float32)
    total += jnp.dot(mask, middle, preferred_element_type=jnp.float32)
    return total + jnp.dot(mask, high, preferred_element_type=jnp.float32)


def cuts(units, weights):
    total, edges = sum(weights), [0]
    for i in range(len(weights)):
        edge = units * sum(weights[:i + 1]) // total
        if edge > edges[-1]:
            edges.append(edge)
    return [(a * UNIT, (b - a) * UNIT) for a, b in zip(edges, edges[1:])]


def plan(nt, ns, cells):
    members = nt * (ns // PLANES)
    units = cells // members // UNIT
    raw = max(units * RAW // 48 // 2, 1)
    return members, raw * UNIT, (units - 2 * raw) * UNIT


def kernel(nt, ns, x_hbm, bucket_hbm, season_hbm, out_ref, calendar, xv, recv, sums, other, y,
           zin, fwd, gath, solved, zret, load_sem, date_sem, own_sem,
           send_a, recv_a, send_b, recv_b, send_s, recv_s, send_y, recv_y, send_o, recv_o,
           send_f, recv_f, send_z, recv_1, recv_2, recv_3, send_g, recv_g,
           send_h, recv_h, send_k, recv_k, send_v, recv_v):
    rows, cells = x_hbm.shape
    w = ns // PLANES
    members, e, mine = plan(nt, ns, cells)
    half = members * e
    start = 2 * half
    chunks = cuts(mine // UNIT, SIZES)
    relays = cuts(half // UNIT, (1,) * RELAYS)
    days = rows * nt * ns
    t, s = lax.axis_index("tm"), lax.axis_index("space")
    q = s // w
    j = s - q * w
    h = q // 2
    me = t * w + j
    mate = q + 1 - 2 * lax.rem(q, 2)
    across = 3 - q
    is_mid = (q == 1) | (q == 2)
    is_outer = jnp.logical_not(is_mid)
    mine_at = pl.multiple_of(start + me * mine, UNIT)
    here_at = pl.multiple_of(h * half, UNIT)
    there_at = pl.multiple_of((1 - h) * half, UNIT)

    def copy(src, dst, send, recv_sem, plane, place=None):
        pt, pj = (t, j) if place is None else place
        return pltpu.make_async_remote_copy(
            src_ref=src, dst_ref=dst, send_sem=send, recv_sem=recv_sem,
            device_id=(pt, plane * w + pj), device_id_type=MESH)

    def settle(ref, sem):
        pltpu.make_async_copy(ref, ref, sem).wait()

    def to_plane(body):
        for dj in range(w):
            for dt in range(nt):
                if dt == dj == 0:
                    continue
                pt, pj = lax.rem(t + dt, nt), lax.rem(j + dj, w)
                body(pt, pj, pt * w + pj)

    load = pltpu.make_async_copy(x_hbm, xv, load_sem)
    load.start()
    dates = [pltpu.make_async_copy(ref, calendar.at[i], date_sem.at[i])
             for i, ref in enumerate((bucket_hbm, season_hbm))]
    for date in dates:
        date.start()
    for k, (a, c) in enumerate(chunks):
        pltpu.make_async_copy(x_hbm.at[:, pl.ds(pl.multiple_of(mine_at + a, UNIT), c)],
                              recv.at[me, :, pl.ds(a, c)], recv_a.at[k]).start()

    @pl.when(is_mid)
    def _():
        pltpu.make_async_copy(x_hbm.at[:, pl.ds(here_at, half)], zin.at[0], own_sem).start()

    barrier = pltpu.get_barrier_semaphore()

    def greet(pt, plane, pj):
        pl.semaphore_signal(barrier, inc=1, device_id=(pt, plane * w + pj), device_id_type=MESH)

    to_plane(lambda pt, pj, p: greet(pt, q, pj))
    greet(t, mate, j)

    @pl.when(is_mid)
    def _():
        greet(t, across, j)
        pl.semaphore_wait(barrier, members + 1)

    @pl.when(is_outer)
    def _():
        pl.semaphore_wait(barrier, members)

    load.wait()

    def push(k):
        a, c = chunks[k]

        def one(pt, pj, p):
            copy(xv.at[:, pl.ds(pl.multiple_of(start + p * mine + a, UNIT), c)],
                 recv.at[me, :, pl.ds(a, c)], send_a, recv_a.at[k], q, (pt, pj)).start()
        to_plane(one)

    def back(k):
        a, c = chunks[k]
        at = pl.ds(pl.multiple_of(mine_at + a, UNIT), c)

        def one(pt, pj, p):
            copy(y.at[p, :, pl.ds(a, c)], out_ref.at[:, at], send_o, recv_o, q, (pt, pj)).start()
        to_plane(one)
        out_ref[:, at] = y[me, :, pl.ds(a, c)]

    def arrived(k):
        a, c = chunks[k]
        settle(recv.at[pl.ds(0, members), :, pl.ds(a, c)], recv_a.at[k])

    push(0)

    @pl.when(is_mid)
    def _():
        copy(xv.at[:, pl.ds(there_at, half)], zin.at[2], send_z, recv_2, across).start()
        for k in range(1, len(chunks)):
            push(k)
        for date in dates:
            date.wait()

        bucket, season = calendar[0], calendar[1]
        key = jnp.where(season < BASE_YEARS, bucket, -1)
        padded = sums.shape[0]

        def planned(count, plane_of):
            order = lax.broadcasted_iota(jnp.int32, (count, days), 0)
            plane, p = plane_of(order)
            day = ((p // w) * ns + plane * w + lax.rem(p, w)) * rows + lax.rem(order, rows)
            pick = day == lax.broadcasted_iota(jnp.int32, (count, days), 1)
            return lambda row: jnp.sum(jnp.where(pick, row, 0), axis=1, keepdims=True)

        here = 2 * members * rows
        of_half = planned(here, lambda order: (
            jnp.where(order < members * rows, q, mate),
            lax.rem(order, members * rows) // rows))
        member = of_half(bucket) == lax.broadcasted_iota(jnp.int32, (here, padded), 1)
        member = jnp.where(member, 1.0, 0.0).astype(jnp.bfloat16)
        key_row = jnp.broadcast_to(of_half(key), (here, here)).T[:1]
        group = lax.broadcasted_iota(jnp.int32, (padded, here), 0)
        baseline = jnp.where(group == key_row, 1.0, 0.0).astype(jnp.bfloat16)
        counted = lax.broadcasted_iota(jnp.int32, (padded, days), 0) == key
        counts = jnp.sum(jnp.where(counted, 1.0, 0.0), axis=1, keepdims=True)
        inverse = 1.0 / jnp.maximum(counts, 1.0)

        def slot_plane(order):
            slot = lax.rem(order // rows, 4)
            plane = jnp.where(slot == 0, q, jnp.where(slot == 1, mate,
                              jnp.where(slot == 2, across, 3 - mate)))
            return plane, order // (4 * rows)

        for i, (a, c) in enumerate(relays):
            settle(fwd.at[:, pl.ds(a, c)], recv_f.at[i])
            copy(fwd.at[:, pl.ds(a, c)], zin.at[3, :, pl.ds(a, c)], send_z, recv_3, across).start()

        def swap(k):
            a, c = chunks[k]
            return copy(sums.at[:, pl.ds(a, c)], other.at[:, pl.ds(a, c)], send_s, recv_s.at[k], across)

        def finish(k):
            a, c = chunks[k]
            cols = pl.ds(a, c)
            swap(k).wait_recv()
            climate = (sums[:, cols] + other[:, cols]) * inverse
            x = recv[:, :, cols].reshape(here, c)
            y[:, :, cols] = (x - exact_dot(member, climate)).reshape(2 * members, rows, c)
            high = pl.ds(members, members)
            copy(y.at[high, :, cols], y.at[pl.ds(0, members), :, cols], send_y, recv_y.at[k], mate).start()
            back(k)

        def spread():
            pltpu.make_async_copy(x_hbm.at[:, pl.ds(here_at, half)], zin.at[0], own_sem).wait()
            for i, sem in enumerate((recv_1, recv_2, recv_3)):
                settle(zin.at[i + 1], sem)

            def one(pt, pj, p):
                copy(zin.at[:, :, pl.ds(pl.multiple_of(p * e, UNIT), e)], gath.at[me],
                     send_g, recv_g, q, (pt, pj)).start()
            to_plane(one)
            gath[me] = zin[:, :, pl.ds(pl.multiple_of(me * e, UNIT), e)]

        def solve():
            of_all = planned(days, slot_plane)
            col = jnp.broadcast_to(of_all(bucket), (days, days))
            based = jnp.broadcast_to(of_all(key), (days, days)).T
            same = jnp.where(col == based, 1.0, 0.0)
            scale = 1.0 / jnp.sum(same, axis=1, keepdims=True)
            settle(gath.at[pl.ds(0, members - 1)], recv_g)
            x = gath[...].reshape(days, e)
            mean = exact_dot(same.astype(jnp.bfloat16), x) * scale
            solved[...] = (x - mean).reshape(members, 4, rows, e)
            at = pl.ds(pl.multiple_of(me * e, UNIT), e)
            out_at = pl.ds(pl.multiple_of(here_at + me * e, UNIT), e)

            def one(pt, pj, p):
                copy(solved.at[p, pl.ds(1, 3)], zret.at[:, :, at], send_h, recv_h, q, (pt, pj)).start()
            to_plane(one)

            def own(pt, pj, p):
                copy(solved.at[p, 0], out_ref.at[:, out_at], send_k, recv_k, q, (pt, pj)).start()
            to_plane(own)
            zret[:, :, at] = solved[me, pl.ds(1, 3)]
            out_ref[:, out_at] = solved[me, 0]

        def home():
            settle(gath.at[pl.ds(0, members - 1), pl.ds(1, 3)], recv_h)
            at = pl.ds(here_at, half)
            for i, plane in ((2, 3 - mate), (1, across), (0, mate)):
                copy(zret.at[i], out_ref.at[:, at], send_v, recv_v, plane).start()

        last = len(chunks) - 1
        for k in range(len(chunks)):
            if k == min(SPREAD, last):
                spread()
            if k == min(SOLVE, last):
                solve()
            arrived(k)
            a, c = chunks[k]
            settle(recv.at[pl.ds(members, members), :, pl.ds(a, c)], recv_b.at[k])
            sums[:, pl.ds(a, c)] = exact_dot(baseline, recv[:, :, pl.ds(a, c)].reshape(here, c))
            swap(k).start()
            if k == last:
                home()
            if k >= LAG:
                finish(k - LAG)
        for k in range(max(len(chunks) - LAG, 0), len(chunks)):
            finish(k)

        settle(sums, send_s)
        settle(y.at[pl.ds(members, members)], send_y)
        settle(zin.at[pl.ds(0, 2)], send_z)
        settle(gath.at[pl.ds(0, members - 1)], send_g)
        settle(gath.at[pl.ds(0, members - 1), pl.ds(1, 3)], send_h)
        settle(gath.at[pl.ds(0, members - 1), 0], send_k)
        settle(gath.at[pl.ds(0, members - 1), 0], recv_k)
        settle(zret, send_v)
        settle(fwd, recv_v)

    @pl.when(is_outer)
    def _():
        for i, (a, c) in enumerate(relays):
            copy(xv.at[:, pl.ds(pl.multiple_of(there_at + a, UNIT), c)], fwd.at[:, pl.ds(a, c)],
                 send_f, recv_f.at[i], mate).start()
        for k in range(1, len(chunks)):
            push(k)
        for k, (a, c) in enumerate(chunks):
            arrived(k)
            copy(recv.at[pl.ds(0, members), :, pl.ds(a, c)], recv.at[pl.ds(members, members), :, pl.ds(a, c)],
                 send_b, recv_b.at[k], mate).start()
            if k == 0:
                copy(xv.at[:, pl.ds(here_at, half)], zin.at[1], send_z, recv_1, mate).start()
        for k, (a, c) in enumerate(chunks):
            settle(y.at[pl.ds(0, members), :, pl.ds(a, c)], recv_y.at[k])
            back(k)

        for date in dates:
            date.wait()
        settle(fwd, send_f)
        settle(fwd, send_z)
        settle(recv.at[pl.ds(0, members)], send_b)
        settle(zin.at[pl.ds(0, 2)], recv_v)

    part = recv.at[pl.ds(0, members - 1)]
    settle(part, send_a)
    settle(part, recv_o)
    settle(part, send_o)


def solution(mesh):
    nt, ns = mesh.shape["tm"], mesh.shape["space"]

    def shards(thermal_field, seasonal_bucket, season_of_record):
        rows, cells = thermal_field.shape
        members, e, mine = plan(nt, ns, cells)
        days, half = rows * nt * ns, members * e
        count = len(cuts(mine // UNIT, SIZES))
        sems = pltpu.SemaphoreType.DMA
        per_chunk = sems((count,))
        vmem = functools.partial(pltpu.VMEM, dtype=jnp.float32)
        return pl.pallas_call(
            functools.partial(kernel, nt, ns),
            out_shape=jax.ShapeDtypeStruct((rows, cells), jnp.float32),
            in_specs=[pl.BlockSpec(memory_space=pltpu.HBM)] * 3,
            out_specs=pl.BlockSpec(memory_space=pltpu.VMEM),
            scratch_shapes=[
                pltpu.VMEM((2, 1, days), jnp.int32),
                vmem((rows, cells)),
                vmem((2 * members, rows, mine)),
                vmem((GROUPS, mine)),
                vmem((GROUPS, mine)),
                vmem((2 * members, rows, mine)),
                vmem((4, rows, half)), vmem((rows, half)),
                vmem((members, 4, rows, e)), vmem((members, 4, rows, e)), vmem((3, rows, half)),
                sems, sems((2,)), sems,
                sems, per_chunk, sems, per_chunk, sems, per_chunk, sems, per_chunk, sems, sems,
                sems, sems((RELAYS,)), sems, sems, sems, sems, sems, sems,
                sems, sems, sems, sems, sems, sems,
            ],
            compiler_params=pltpu.CompilerParams(
                collective_id=0, has_side_effects=True, vmem_limit_bytes=56 * 2**20),
            name="anomaly",
        )(*(pltpu.with_memory_space_constraint(a, pltpu.HBM) for a in (
            thermal_field, seasonal_bucket.reshape(1, -1), season_of_record.reshape(1, -1))))

    placed = (P(("tm", "space"), None), P(), P())
    return jax.shard_map(
        shards, mesh=mesh, in_specs=placed, out_specs=P(("tm", "space"), None), check_vma=False
    )
```

```python
import functools

import jax
import jax.numpy as jnp
from jax import lax
from jax.experimental import pallas as pl
from jax.experimental.pallas import tpu as pltpu
from jax.sharding import PartitionSpec as P

GROUPS = 46
BASE_YEARS = 6
PLANES = 4
UNIT = 128
RAW = 12
SIZES = (2, 3, 3, 3, 3, 3, 3, 3, 3, 3, 3, 2, 2)
LAG = 3
RELAY = 2
AHEAD = 20
FORWARD = 3
SPREAD = 5
SOLVE = 9
OWN = 3
DIRECT = 2
MESH = pl.DeviceIdType.MESH


def exact_dot(mask, x):
    high = x.astype(jnp.bfloat16)
    rest = x - high.astype(jnp.float32)
    middle = rest.astype(jnp.bfloat16)
    low = (rest - middle.astype(jnp.float32)).astype(jnp.bfloat16)
    total = jnp.dot(mask, low, preferred_element_type=jnp.float32)
    total += jnp.dot(mask, middle, preferred_element_type=jnp.float32)
    return total + jnp.dot(mask, high, preferred_element_type=jnp.float32)


def cuts(units, weights):
    total, edges = sum(weights), [0]
    for i in range(len(weights)):
        edge = units * sum(weights[:i + 1]) // total
        if edge > edges[-1]:
            edges.append(edge)
    return [(a * UNIT, (b - a) * UNIT) for a, b in zip(edges, edges[1:])]


def plan(nt, ns, cells):
    members = nt * (ns // PLANES)
    units = cells // members // UNIT
    raw = max(units * RAW // 48 // 2, 1)
    return members, raw * UNIT, (units - 2 * raw) * UNIT


def kernel(nt, ns, x_hbm, bucket_hbm, season_hbm, out_ref, calendar, xv, recv, sums, other, y,
           zin, fwd, gath, solved, load_sem, date_sem, own_sem,
           send_a, recv_a, send_b, recv_b, send_s, recv_s, send_o, recv_o,
           send_f, recv_f, send_z, recv_1, recv_2, recv_3, send_g, recv_g,
           send_k, recv_k, send_v, recv_v):
    rows, cells = x_hbm.shape
    w = ns // PLANES
    members, e, mine = plan(nt, ns, cells)
    half = members * e
    start = 2 * half
    chunks = cuts(mine // UNIT, SIZES)
    direct = min(DIRECT, len(chunks) - 1)
    days = rows * nt * ns
    t, s = lax.axis_index("tm"), lax.axis_index("space")
    q = s // w
    j = s - q * w
    h = q // 2
    me = t * w + j
    mate = q + 1 - 2 * lax.rem(q, 2)
    across = 3 - q
    is_mid = (q == 1) | (q == 2)
    is_outer = jnp.logical_not(is_mid)
    mine_at = pl.multiple_of(start + me * mine, UNIT)
    here_at = pl.multiple_of(h * half, UNIT)
    there_at = pl.multiple_of((1 - h) * half, UNIT)

    def copy(src, dst, send, recv_sem, plane, place=None):
        pt, pj = (t, j) if place is None else place
        return pltpu.make_async_remote_copy(
            src_ref=src, dst_ref=dst, send_sem=send, recv_sem=recv_sem,
            device_id=(pt, plane * w + pj), device_id_type=MESH)

    def settle(ref, sem):
        pltpu.make_async_copy(ref, ref, sem).wait()

    def to_plane(body, own=False):
        for dj in range(w):
            for dt in range(nt):
                if dt == dj == 0 and not own:
                    continue
                pt, pj = lax.rem(t + dt, nt), lax.rem(j + dj, w)
                body(pt, pj, pt * w + pj)

    load = pltpu.make_async_copy(x_hbm, xv, load_sem)
    load.start()
    dates = [pltpu.make_async_copy(ref, calendar.at[i], date_sem.at[i])
             for i, ref in enumerate((bucket_hbm, season_hbm))]
    for date in dates:
        date.start()

    def keep(k):
        a, c = chunks[k]
        pltpu.make_async_copy(x_hbm.at[:, pl.ds(pl.multiple_of(mine_at + a, UNIT), c)],
                              recv.at[me, :, pl.ds(a, c)], recv_a.at[k]).start()
    for k in range(direct, len(chunks)):
        keep(k)

    @pl.when(is_mid)
    def _():
        for k in range(direct):
            keep(k)
        pltpu.make_async_copy(x_hbm.at[:, pl.ds(here_at, half)], zin.at[0], own_sem).start()

    barrier = pltpu.get_barrier_semaphore()

    def greet(pt, plane, pj):
        pl.semaphore_signal(barrier, inc=1, device_id=(pt, plane * w + pj), device_id_type=MESH)

    to_plane(lambda pt, pj, p: greet(pt, q, pj))

    @pl.when(is_mid)
    def _():
        to_plane(lambda pt, pj, p: greet(pt, mate, pj), True)
        greet(t, across, j)
        pl.semaphore_wait(barrier, members)

    @pl.when(is_outer)
    def _():
        pl.semaphore_wait(barrier, 2 * members - 1)

    load.wait()

    def push(k):
        a, c = chunks[k]

        def one(pt, pj, p):
            copy(xv.at[:, pl.ds(pl.multiple_of(start + p * mine + a, UNIT), c)],
                 recv.at[me, :, pl.ds(a, c)], send_a, recv_a.at[k], q, (pt, pj)).start()
        to_plane(one)

    def back(k):
        a, c = chunks[k]
        at = pl.ds(pl.multiple_of(mine_at + a, UNIT), c)

        def far(pt, pj, p):
            copy(y.at[members + p, :, pl.ds(a, c)], out_ref.at[:, at], send_o, recv_o, mate, (pt, pj)).start()

        def near(pt, pj, p):
            copy(y.at[p, :, pl.ds(a, c)], out_ref.at[:, at], send_o, recv_o, q, (pt, pj)).start()
        to_plane(far, True)
        to_plane(near)
        out_ref[:, at] = y[me, :, pl.ds(a, c)]

    def arrived(k):
        a, c = chunks[k]
        settle(recv.at[pl.ds(0, members), :, pl.ds(a, c)], recv_a.at[k])

    @pl.when(is_mid)
    def _():
        push(0)
        copy(xv.at[:, pl.ds(there_at, half)], zin.at[2], send_z, recv_2, across).start()
        for k in range(1, min(AHEAD, len(chunks))):
            push(k)
        for date in dates:
            date.wait()

        bucket, season = calendar[0], calendar[1]
        key = jnp.where(season < BASE_YEARS, bucket, -1)
        padded = sums.shape[0]

        def planned(count, plane_of):
            order = lax.broadcasted_iota(jnp.int32, (count, days), 0)
            plane, p = plane_of(order)
            day = ((p // w) * ns + plane * w + lax.rem(p, w)) * rows + lax.rem(order, rows)
            pick = day == lax.broadcasted_iota(jnp.int32, (count, days), 1)
            return lambda row: jnp.sum(jnp.where(pick, row, 0), axis=1, keepdims=True)

        here = 2 * members * rows
        of_half = planned(here, lambda order: (
            jnp.where(order < members * rows, q, mate),
            lax.rem(order, members * rows) // rows))
        member = of_half(bucket) == lax.broadcasted_iota(jnp.int32, (here, padded), 1)
        member = jnp.where(member, 1.0, 0.0).astype(jnp.bfloat16)
        key_row = jnp.broadcast_to(of_half(key), (here, here)).T[:1]
        group = lax.broadcasted_iota(jnp.int32, (padded, here), 0)
        baseline = jnp.where(group == key_row, 1.0, 0.0).astype(jnp.bfloat16)
        counted = lax.broadcasted_iota(jnp.int32, (padded, days), 0) == key
        counts = jnp.sum(jnp.where(counted, 1.0, 0.0), axis=1, keepdims=True)
        inverse = 1.0 / jnp.maximum(counts, 1.0)

        def slot_plane(order):
            slot = lax.rem(order // rows, 4)
            plane = jnp.where(slot == 0, q, jnp.where(slot == 1, mate,
                              jnp.where(slot == 2, across, 3 - mate)))
            return plane, order // (4 * rows)

        def relay():
            settle(fwd, recv_f)
            copy(fwd, zin.at[3], send_z, recv_3, across).start()

        def swap(k):
            a, c = chunks[k]
            return copy(sums.at[:, pl.ds(a, c)], other.at[:, pl.ds(a, c)], send_s, recv_s.at[k], across)

        def finish(k):
            a, c = chunks[k]
            cols = pl.ds(a, c)
            swap(k).wait_recv()
            climate = (sums[:, cols] + other[:, cols]) * inverse
            x = recv[:, :, cols].reshape(here, c)
            y[:, :, cols] = (x - exact_dot(member, climate)).reshape(2 * members, rows, c)
            back(k)

        def spread():
            pltpu.make_async_copy(x_hbm.at[:, pl.ds(here_at, half)], zin.at[0], own_sem).wait()
            for i, sem in enumerate((recv_1, recv_2, recv_3)):
                settle(zin.at[i + 1], sem)

            def one(pt, pj, p):
                copy(zin.at[:, :, pl.ds(pl.multiple_of(p * e, UNIT), e)], gath.at[me],
                     send_g, recv_g, q, (pt, pj)).start()
            to_plane(one)
            gath[me] = zin[:, :, pl.ds(pl.multiple_of(me * e, UNIT), e)]

        solved_at = pl.ds(pl.multiple_of(here_at + me * e, UNIT), e)

        def send_home(slot, plane, own, send, recv_sem):
            def one(pt, pj, p):
                copy(solved.at[p, slot], out_ref.at[:, solved_at], send, recv_sem, plane, (pt, pj)).start()
            to_plane(one, own)

        def solve():
            of_all = planned(days, slot_plane)
            col = jnp.broadcast_to(of_all(bucket), (days, days))
            based = jnp.broadcast_to(of_all(key), (days, days)).T
            same = jnp.where(col == based, 1.0, 0.0)
            scale = 1.0 / jnp.sum(same, axis=1, keepdims=True)
            settle(gath.at[pl.ds(0, members - 1)], recv_g)
            x = gath[...].reshape(days, e)
            mean = exact_dot(same.astype(jnp.bfloat16), x) * scale
            solved[...] = (x - mean).reshape(members, 4, rows, e)
            send_home(1, mate, True, send_k, recv_k)
            send_home(0, q, False, send_k, recv_k)
            out_ref[:, solved_at] = solved[me, 0]

        last = len(chunks) - 1
        for k in range(len(chunks)):
            if k + AHEAD < len(chunks):
                push(k + AHEAD)
            if k == min(RELAY, last):
                relay()
            if k == min(SPREAD, last):
                spread()
            if k == min(SOLVE, last):
                solve()
            arrived(k)
            a, c = chunks[k]
            settle(recv.at[pl.ds(members, members), :, pl.ds(a, c)], recv_b.at[k])
            sums[:, pl.ds(a, c)] = exact_dot(baseline, recv[:, :, pl.ds(a, c)].reshape(here, c))
            swap(k).start()
            if k == last:
                send_home(3, 3 - mate, True, send_v, recv_v)
                send_home(2, across, True, send_v, recv_v)
            if k >= LAG:
                finish(k - LAG)
        for k in range(max(len(chunks) - LAG, 0), len(chunks)):
            finish(k)

        settle(sums, send_s)
        settle(zin.at[pl.ds(0, 2)], send_z)
        settle(gath.at[pl.ds(0, members - 1)], send_g)
        settle(gath.at[:, 0], send_k)
        settle(gath.at[pl.ds(0, members - 1), 0], send_k)
        settle(gath.at[pl.ds(0, members - 1), 0], recv_k)
        settle(gath.at[:, pl.ds(0, 2)], send_v)
        settle(y.at[pl.ds(0, 2 * members - 1)], send_o)
        settle(recv.at[pl.ds(0, members - 1)], recv_o)
        settle(recv.at[pl.ds(0, members - 1)], send_a)

    @pl.when(is_outer)
    def _():
        for k, (a, c) in enumerate(chunks[:direct]):
            def one(pt, pj, p):
                copy(xv.at[:, pl.ds(pl.multiple_of(start + p * mine + a, UNIT), c)],
                     recv.at[members + me, :, pl.ds(a, c)], send_b, recv_b.at[k], mate, (pt, pj)).start()
            to_plane(one, True)
            if k == min(FORWARD, direct - 1):
                copy(xv.at[:, pl.ds(there_at, half)], fwd, send_f, recv_f, mate).start()
        for k in range(direct, len(chunks)):
            push(k)
        for k in range(direct, len(chunks)):
            a, c = chunks[k]
            arrived(k)
            copy(recv.at[pl.ds(0, members), :, pl.ds(a, c)], recv.at[pl.ds(members, members), :, pl.ds(a, c)],
                 send_b, recv_b.at[k], mate).start()
            if k == max(direct, min(OWN, len(chunks) - 1)):
                copy(xv.at[:, pl.ds(here_at, half)], zin.at[1], send_z, recv_1, mate).start()
        for date in dates:
            date.wait()
        settle(fwd, send_f)
        settle(fwd, send_z)
        settle(recv.at[pl.ds(0, members)], send_b)
        settle(recv.at[pl.ds(0, members - 1), :, pl.ds(chunks[direct][0], mine - chunks[direct][0])], send_a)
        settle(gath.at[:, 0], recv_k)
        settle(recv.at[pl.ds(0, members)], recv_o)

    settle(fwd, recv_v)


def solution(mesh):
    nt, ns = mesh.shape["tm"], mesh.shape["space"]

    def shards(thermal_field, seasonal_bucket, season_of_record):
        rows, cells = thermal_field.shape
        members, e, mine = plan(nt, ns, cells)
        days, half = rows * nt * ns, members * e
        count = len(cuts(mine // UNIT, SIZES))
        sems = pltpu.SemaphoreType.DMA
        per_chunk = sems((count,))
        vmem = functools.partial(pltpu.VMEM, dtype=jnp.float32)
        return pl.pallas_call(
            functools.partial(kernel, nt, ns),
            out_shape=jax.ShapeDtypeStruct((rows, cells), jnp.float32),
            in_specs=[pl.BlockSpec(memory_space=pltpu.HBM)] * 3,
            out_specs=pl.BlockSpec(memory_space=pltpu.VMEM),
            scratch_shapes=[
                pltpu.VMEM((2, 1, days), jnp.int32),
                vmem((rows, cells)),
                vmem((2 * members, rows, mine)),
                vmem((GROUPS, mine)),
                vmem((GROUPS, mine)),
                vmem((2 * members, rows, mine)),
                vmem((4, rows, half)), vmem((rows, half)),
                vmem((members, 4, rows, e)), vmem((members, 4, rows, e)),
                sems, sems((2,)), sems,
                sems, per_chunk, sems, per_chunk, sems, per_chunk, sems, sems,
                sems, sems, sems, sems, sems, sems, sems, sems,
                sems, sems, sems, sems,
            ],
            compiler_params=pltpu.CompilerParams(
                collective_id=0, has_side_effects=True, vmem_limit_bytes=30 * 2**20),
            name="anomaly",
        )(*(pltpu.with_memory_space_constraint(a, pltpu.HBM) for a in (
            thermal_field, seasonal_bucket.reshape(1, -1), season_of_record.reshape(1, -1))))

    placed = (P(("tm", "space"), None), P(), P())
    return jax.shard_map(
        shards, mesh=mesh, in_specs=placed, out_specs=P(("tm", "space"), None), check_vma=False
    )
```

```python
import functools

import jax
import jax.numpy as jnp
from jax import lax
from jax.experimental import pallas as pl
from jax.experimental.pallas import tpu as pltpu
from jax.sharding import PartitionSpec as P

GROUPS = 46
BASE_YEARS = 6
PLANES = 4
UNIT = 128
RAW = 8
SIZES = (2, 3, 3, 3, 3, 3, 3, 3, 3, 3, 3, 2, 2)
PIECES = 4
DIRECT = 2
LAG = 3
RAW_SENT = 0
RAW_FROM = 5
RAW_EVERY = 2
MESH = pl.DeviceIdType.MESH


def exact_dot(mask, x):
    high = x.astype(jnp.bfloat16)
    rest = x - high.astype(jnp.float32)
    middle = rest.astype(jnp.bfloat16)
    low = (rest - middle.astype(jnp.float32)).astype(jnp.bfloat16)
    total = jnp.dot(mask, low, preferred_element_type=jnp.float32)
    total += jnp.dot(mask, middle, preferred_element_type=jnp.float32)
    return total + jnp.dot(mask, high, preferred_element_type=jnp.float32)


def cuts(start, units, weights):
    total, edges = sum(weights), [0]
    for i in range(len(weights)):
        edge = units * sum(weights[:i + 1]) // total
        if edge > edges[-1]:
            edges.append(edge)
    return [(start + a * UNIT, (b - a) * UNIT) for a, b in zip(edges, edges[1:])]


def plan(nt, ns, cells):
    members = nt * (ns // PLANES)
    units = cells // members // UNIT
    raw = max(units * RAW // 48, 1)
    swapped = cuts(0, units - raw, SIZES)
    return members, units * UNIT, raw * UNIT, swapped, cuts((units - raw) * UNIT, raw, (1,) * PIECES)


def kernel(nt, ns, x_hbm, bucket_hbm, season_hbm, out_ref, calendar, xv, recv, sums, other, y, far,
           load_sem, date_sem, send_a, recv_a, send_b, recv_b, send_s, recv_s, send_o, recv_o,
           send_r, recv_r):
    rows, cells = x_hbm.shape
    w = ns // PLANES
    members, mine, e, swapped, raws = plan(nt, ns, cells)
    chunks = swapped + raws
    last = len(swapped) - 1
    order = []
    for k in range(len(swapped)):
        order.append(k)
        order += [len(swapped) + i for i in range(len(raws))
                  if min(RAW_FROM + i * RAW_EVERY, last) == k]
    direct = min(DIRECT, len(swapped) - 1)
    days = rows * nt * ns
    t, s = lax.axis_index("tm"), lax.axis_index("space")
    q = s // w
    j = s - q * w
    me = t * w + j
    mate = q + 1 - 2 * lax.rem(q, 2)
    across = 3 - q
    beyond = 3 - mate
    is_mid = (q == 1) | (q == 2)
    is_outer = jnp.logical_not(is_mid)
    mine_at = pl.multiple_of(me * mine, UNIT)

    def copy(src, dst, send, recv_sem, plane, place):
        pt, pj = place
        return pltpu.make_async_remote_copy(
            src_ref=src, dst_ref=dst, send_sem=send, recv_sem=recv_sem,
            device_id=(pt, plane * w + pj), device_id_type=MESH)

    def settle(ref, sem):
        pltpu.make_async_copy(ref, ref, sem).wait()

    def to_plane(body, own=False):
        for dj in range(w):
            for dt in range(nt):
                if dt == dj == 0 and not own:
                    continue
                pt, pj = lax.rem(t + dt, nt), lax.rem(j + dj, w)
                body(pt, pj, pt * w + pj)

    load = pltpu.make_async_copy(x_hbm, xv, load_sem)
    load.start()
    barrier = pltpu.get_barrier_semaphore()

    def greet(plane, own):
        def one(pt, pj, p):
            pl.semaphore_signal(barrier, inc=1, device_id=(pt, plane * w + pj), device_id_type=MESH)
        to_plane(one, own)

    greet(q, False)

    @pl.when(is_mid)
    def _():
        for plane in (across, mate, beyond):
            greet(plane, True)

    dates = [pltpu.make_async_copy(ref, calendar.at[i], date_sem.at[i])
             for i, ref in enumerate((bucket_hbm, season_hbm))]

    def keep(k):
        a, c = chunks[k]
        pltpu.make_async_copy(x_hbm.at[:, pl.ds(pl.multiple_of(mine_at + a, UNIT), c)],
                              recv.at[me, :, pl.ds(a, c)], recv_a.at[k]).start()

    for k in order[direct:]:
        keep(k)

    def part(p, a, c):
        return xv.at[:, pl.ds(pl.multiple_of(p * mine + a, UNIT), c)]

    def push(k):
        a, c = chunks[k]

        def one(pt, pj, p):
            copy(part(p, a, c), recv.at[me, :, pl.ds(a, c)], send_a, recv_a.at[k], q, (pt, pj)).start()
        to_plane(one)

    def arrived(k):
        a, c = chunks[k]
        settle(recv.at[pl.ds(0, members), :, pl.ds(a, c)], recv_a.at[k])

    def send_raw(plane, slot):
        def one(pt, pj, p):
            copy(part(p, mine - e, e), far.at[slot], send_r, recv_r, plane, (pt, pj)).start()
        to_plane(one, True)

    @pl.when(is_mid)
    def _():
        for k in range(direct):
            keep(k)
        for date in dates:
            date.start()
        pl.semaphore_wait(barrier, 2 * members - 1)
        load.wait()
        push(0)
        send_raw(across, me)
        for k in order[1:]:
            push(k)
        for date in dates:
            date.wait()

        bucket, season = calendar[0], calendar[1]
        key = jnp.where(season < BASE_YEARS, bucket, -1)
        padded = sums.shape[0]
        here = 2 * members * rows

        def half(first, second):
            order = lax.broadcasted_iota(jnp.int32, (here, days), 0)
            plane = jnp.where(order < members * rows, first, second)
            p = lax.rem(order, members * rows) // rows
            day = ((p // w) * ns + plane * w + lax.rem(p, w)) * rows + lax.rem(order, rows)
            pick = day == lax.broadcasted_iota(jnp.int32, (here, days), 1)
            return lambda row: jnp.sum(jnp.where(pick, row, 0), axis=1, keepdims=True)

        def baseline(of_half):
            key_row = jnp.broadcast_to(of_half(key), (here, here)).T[:1]
            group = lax.broadcasted_iota(jnp.int32, (padded, here), 0)
            return jnp.where(group == key_row, 1.0, 0.0).astype(jnp.bfloat16)

        ours = half(q, mate)
        member = ours(bucket) == lax.broadcasted_iota(jnp.int32, (here, padded), 1)
        member = jnp.where(member, 1.0, 0.0).astype(jnp.bfloat16)
        of_ours, of_theirs = baseline(ours), baseline(half(across, beyond))
        counted = lax.broadcasted_iota(jnp.int32, (padded, days), 0) == key
        counts = jnp.sum(jnp.where(counted, 1.0, 0.0), axis=1, keepdims=True)
        inverse = 1.0 / jnp.maximum(counts, 1.0)

        def total(k):
            a, c = chunks[k]
            arrived(k)
            settle(recv.at[pl.ds(members, members), :, pl.ds(a, c)], recv_b.at[k])
            return exact_dot(of_ours, recv[:, :, pl.ds(a, c)].reshape(here, c))

        def swap(k):
            a, c = chunks[k]
            return copy(sums.at[:, pl.ds(a, c)], other.at[:, pl.ds(a, c)], send_s, recv_s.at[k], across, (t, j))

        def back(k, both):
            a, c = chunks[k]
            cols = pl.ds(a, c)
            at = pl.ds(pl.multiple_of(mine_at + a, UNIT), c)
            x = recv[:, :, cols].reshape(here, c)
            y[:, :, cols] = (x - exact_dot(member, both * inverse)).reshape(2 * members, rows, c)

            def outer(pt, pj, p):
                copy(y.at[members + p, :, cols], out_ref.at[:, at], send_o, recv_o, mate, (pt, pj)).start()

            def near(pt, pj, p):
                copy(y.at[p, :, cols], out_ref.at[:, at], send_o, recv_o, q, (pt, pj)).start()
            to_plane(outer, True)
            to_plane(near)
            out_ref[:, at] = y[me, :, cols]

        def finish(k):
            a, c = chunks[k]
            swap(k).wait_recv()
            back(k, sums[:, pl.ds(a, c)] + other[:, pl.ds(a, c)])

        def finish_raw(k):
            a, c = chunks[k]
            if k == len(swapped):
                settle(far, recv_r)
            theirs = far[:, :, pl.ds(a - (mine - e), c)].reshape(here, c)
            back(k, total(k) + exact_dot(of_theirs, theirs))

        for k in order:
            if k > last:
                finish_raw(k)
                continue
            a, c = chunks[k]
            sums[:, pl.ds(a, c)] = total(k)
            swap(k).start()
            if k >= LAG:
                finish(k - LAG)
        for k in range(max(len(swapped) - LAG, 0), len(swapped)):
            finish(k)

        settle(sums, send_s)
        settle(far.at[pl.ds(0, members)], send_r)
        settle(y.at[pl.ds(0, 2 * members - 1)], send_o)
        settle(recv.at[pl.ds(0, members - 1)], recv_o)
        settle(recv.at[pl.ds(0, members - 1)], send_a)

    @pl.when(is_outer)
    def _():
        pl.semaphore_wait(barrier, 3 * members - 1)
        load.wait()
        for k, (a, c) in enumerate(chunks[:direct]):
            def one(pt, pj, p):
                copy(part(p, a, c), recv.at[members + me, :, pl.ds(a, c)],
                     send_b, recv_b.at[k], mate, (pt, pj)).start()
            to_plane(one, True)
        for k in order[direct:]:
            push(k)
        for i, k in enumerate(order[direct:]):
            a, c = chunks[k]
            if i == min(RAW_SENT, last - direct):
                send_raw(beyond, members + me)
            arrived(k)
            copy(recv.at[pl.ds(0, members), :, pl.ds(a, c)], recv.at[pl.ds(members, members), :, pl.ds(a, c)],
                 send_b, recv_b.at[k], mate, (t, j)).start()
        settle(far.at[pl.ds(0, members)], send_r)
        settle(recv.at[pl.ds(0, members)], send_b)
        settle(recv.at[pl.ds(0, members - 1), :, pl.ds(chunks[direct][0], mine - chunks[direct][0])], send_a)
        settle(recv.at[pl.ds(0, members)], recv_o)


def solution(mesh):
    nt, ns = mesh.shape["tm"], mesh.shape["space"]

    def shards(thermal_field, seasonal_bucket, season_of_record):
        rows, cells = thermal_field.shape
        members, mine, e, swapped, raws = plan(nt, ns, cells)
        days = rows * nt * ns
        sems = pltpu.SemaphoreType.DMA
        per_chunk, per_swap = sems((len(swapped) + len(raws),)), sems((len(swapped),))
        vmem = functools.partial(pltpu.VMEM, dtype=jnp.float32)
        return pl.pallas_call(
            functools.partial(kernel, nt, ns),
            out_shape=jax.ShapeDtypeStruct((rows, cells), jnp.float32),
            in_specs=[pl.BlockSpec(memory_space=pltpu.HBM)] * 3,
            out_specs=pl.BlockSpec(memory_space=pltpu.VMEM),
            scratch_shapes=[
                pltpu.VMEM((2, 1, days), jnp.int32),
                vmem((rows, cells)),
                vmem((2 * members, rows, mine)),
                vmem((GROUPS, mine - e)),
                vmem((GROUPS, mine - e)),
                vmem((2 * members, rows, mine)),
                vmem((2 * members, rows, e)),
                sems, sems((2,)),
                sems, per_chunk, sems, per_chunk, sems, per_swap, sems, sems,
                sems, sems,
            ],
            compiler_params=pltpu.CompilerParams(
                collective_id=0, has_side_effects=True, vmem_limit_bytes=30 * 2**20),
            name="anomaly",
        )(*(pltpu.with_memory_space_constraint(a, pltpu.HBM) for a in (
            thermal_field, seasonal_bucket.reshape(1, -1), season_of_record.reshape(1, -1))))

    placed = (P(("tm", "space"), None), P(), P())
    return jax.shard_map(
        shards, mesh=mesh, in_specs=placed, out_specs=P(("tm", "space"), None), check_vma=False
    )
```

```python
import functools

import jax
import jax.numpy as jnp
from jax import lax
from jax.experimental import pallas as pl
from jax.experimental.pallas import tpu as pltpu
from jax.sharding import PartitionSpec as P

GROUPS = 46
BASE_YEARS = 6
PLANES = 4
UNIT = 128
RAW = 8
SIZES = (2, 3, 3, 4, 4, 4, 4, 4, 4, 3, 2, 1)
PIECES = 4
DIRECT = 2
LAG = 3
RAW_SENT = 0
RAW_FROM = 5
RAW_EVERY = 2
MESH = pl.DeviceIdType.MESH


def exact_dot(mask, x):
    high = x.astype(jnp.bfloat16)
    rest = x - high.astype(jnp.float32)
    middle = rest.astype(jnp.bfloat16)
    low = (rest - middle.astype(jnp.float32)).astype(jnp.bfloat16)
    total = jnp.dot(mask, low, preferred_element_type=jnp.float32)
    total += jnp.dot(mask, middle, preferred_element_type=jnp.float32)
    return total + jnp.dot(mask, high, preferred_element_type=jnp.float32)


def cuts(start, units, weights):
    total, edges = sum(weights), [0]
    for i in range(len(weights)):
        edge = units * sum(weights[:i + 1]) // total
        if edge > edges[-1]:
            edges.append(edge)
    return [(start + a * UNIT, (b - a) * UNIT) for a, b in zip(edges, edges[1:])]


def plan(nt, ns, cells):
    members = nt * (ns // PLANES)
    units = cells // members // UNIT
    raw = max(units * RAW // 48, 1)
    swapped = cuts(0, units - raw, SIZES)
    return members, units * UNIT, raw * UNIT, swapped, cuts((units - raw) * UNIT, raw, (1,) * PIECES)


def kernel(nt, ns, x_hbm, bucket_hbm, season_hbm, out_ref, calendar, xv, recv, sums, other, y, far,
           load_sem, date_sem, send_a, recv_a, send_b, send_s, recv_s, send_o, recv_o,
           send_r, recv_r):
    rows, cells = x_hbm.shape
    w = ns // PLANES
    members, mine, e, swapped, raws = plan(nt, ns, cells)
    chunks = swapped + raws
    last = len(swapped) - 1
    order = []
    for k in range(len(swapped)):
        order.append(k)
        order += [len(swapped) + i for i in range(len(raws))
                  if min(RAW_FROM + i * RAW_EVERY, last) == k]
    direct = min(DIRECT, len(swapped) - 1)
    days = rows * nt * ns
    t, s = lax.axis_index("tm"), lax.axis_index("space")
    q = s // w
    j = s - q * w
    me = t * w + j
    mate = q + 1 - 2 * lax.rem(q, 2)
    across = 3 - q
    beyond = 3 - mate
    is_mid = (q == 1) | (q == 2)
    is_outer = jnp.logical_not(is_mid)
    mine_at = pl.multiple_of(me * mine, UNIT)

    def copy(src, dst, send, recv_sem, plane, place):
        pt, pj = place
        return pltpu.make_async_remote_copy(
            src_ref=src, dst_ref=dst, send_sem=send, recv_sem=recv_sem,
            device_id=(pt, plane * w + pj), device_id_type=MESH)

    def settle(ref, sem):
        pltpu.make_async_copy(ref, ref, sem).wait()

    def to_plane(body, own=False):
        for dj in range(w):
            for dt in range(nt):
                if dt == dj == 0 and not own:
                    continue
                pt, pj = lax.rem(t + dt, nt), lax.rem(j + dj, w)
                body(pt, pj, pt * w + pj)

    load = pltpu.make_async_copy(x_hbm, xv, load_sem)
    load.start()
    barrier = pltpu.get_barrier_semaphore()

    def greet(plane, own):
        def one(pt, pj, p):
            pl.semaphore_signal(barrier, inc=1, device_id=(pt, plane * w + pj), device_id_type=MESH)
        to_plane(one, own)

    greet(q, False)

    @pl.when(is_mid)
    def _():
        for plane in (across, mate, beyond):
            greet(plane, True)

    dates = [pltpu.make_async_copy(ref, calendar.at[i], date_sem.at[i])
             for i, ref in enumerate((bucket_hbm, season_hbm))]

    def keep(k):
        a, c = chunks[k]
        pltpu.make_async_copy(x_hbm.at[:, pl.ds(pl.multiple_of(mine_at + a, UNIT), c)],
                              recv.at[me, :, pl.ds(a, c)], recv_a.at[k]).start()

    for k in order[direct:]:
        keep(k)

    def part(p, a, c):
        return xv.at[:, pl.ds(pl.multiple_of(p * mine + a, UNIT), c)]

    def push(k):
        a, c = chunks[k]

        def one(pt, pj, p):
            copy(part(p, a, c), recv.at[me, :, pl.ds(a, c)], send_a, recv_a.at[k], q, (pt, pj)).start()
        to_plane(one)

    def send_raw(plane, slot):
        def one(pt, pj, p):
            copy(part(p, mine - e, e), far.at[slot], send_r, recv_r, plane, (pt, pj)).start()
        to_plane(one, True)

    @pl.when(is_mid)
    def _():
        for k in range(direct):
            keep(k)
        for date in dates:
            date.start()
        pl.semaphore_wait(barrier, 2 * members - 1)
        load.wait()
        push(0)
        send_raw(across, me)
        for k in order[1:]:
            push(k)
        for date in dates:
            date.wait()

        bucket, season = calendar[0], calendar[1]
        key = jnp.where(season < BASE_YEARS, bucket, -1)
        padded = sums.shape[0]
        here = 2 * members * rows

        def half(first, second):
            order = lax.broadcasted_iota(jnp.int32, (here, days), 0)
            plane = jnp.where(order < members * rows, first, second)
            p = lax.rem(order, members * rows) // rows
            day = ((p // w) * ns + plane * w + lax.rem(p, w)) * rows + lax.rem(order, rows)
            pick = day == lax.broadcasted_iota(jnp.int32, (here, days), 1)
            return lambda row: jnp.sum(jnp.where(pick, row, 0), axis=1, keepdims=True)

        def baseline(of_half):
            key_row = jnp.broadcast_to(of_half(key), (here, here)).T[:1]
            group = lax.broadcasted_iota(jnp.int32, (padded, here), 0)
            return jnp.where(group == key_row, 1.0, 0.0).astype(jnp.bfloat16)

        ours = half(q, mate)
        member = ours(bucket) == lax.broadcasted_iota(jnp.int32, (here, padded), 1)
        member = jnp.where(member, 1.0, 0.0).astype(jnp.bfloat16)
        of_ours, of_theirs = baseline(ours), baseline(half(across, beyond))
        counted = lax.broadcasted_iota(jnp.int32, (padded, days), 0) == key
        counts = jnp.sum(jnp.where(counted, 1.0, 0.0), axis=1, keepdims=True)
        inverse = 1.0 / jnp.maximum(counts, 1.0)

        def total(k):
            a, c = chunks[k]
            settle(recv.at[:, :, pl.ds(a, c)], recv_a.at[k])
            return exact_dot(of_ours, recv[:, :, pl.ds(a, c)].reshape(here, c))

        def swap(k):
            a, c = chunks[k]
            return copy(sums.at[:, pl.ds(a, c)], other.at[:, pl.ds(a, c)], send_s, recv_s.at[k], across, (t, j))

        def back(k, both):
            a, c = chunks[k]
            cols = pl.ds(a, c)
            at = pl.ds(pl.multiple_of(mine_at + a, UNIT), c)
            x = recv[:, :, cols].reshape(here, c)
            y[:, :, cols] = (x - exact_dot(member, both * inverse)).reshape(2 * members, rows, c)

            for p in range(members):
                copy(y.at[members + p, :, cols], out_ref.at[:, at], send_o, recv_o, mate, (p // w, p % w)).start()

            def near(pt, pj, p):
                copy(y.at[p, :, cols], out_ref.at[:, at], send_o, recv_o, q, (pt, pj)).start()
            to_plane(near)
            out_ref[:, at] = y[me, :, cols]

        def finish(k):
            a, c = chunks[k]
            swap(k).wait_recv()
            back(k, sums[:, pl.ds(a, c)] + other[:, pl.ds(a, c)])

        def finish_raw(k):
            a, c = chunks[k]
            if k == len(swapped):
                settle(far, recv_r)
            theirs = far[:, :, pl.ds(a - (mine - e), c)].reshape(here, c)
            back(k, total(k) + exact_dot(of_theirs, theirs))

        for k in order:
            if k > last:
                finish_raw(k)
                continue
            a, c = chunks[k]
            sums[:, pl.ds(a, c)] = total(k)
            swap(k).start()
            if k >= LAG:
                finish(k - LAG)
        for k in range(max(len(swapped) - LAG, 0), len(swapped)):
            finish(k)

        settle(sums, send_s)
        settle(far.at[pl.ds(0, members)], send_r)
        settle(y.at[pl.ds(0, 2 * members - 1)], send_o)
        settle(recv.at[pl.ds(0, members - 1)], recv_o)
        settle(recv.at[pl.ds(0, members - 1)], send_a)

    @pl.when(is_outer)
    def _():
        pl.semaphore_wait(barrier, 3 * members - 1)
        load.wait()
        for k, (a, c) in enumerate(chunks[:direct]):
            def one(pt, pj, p):
                copy(part(p, a, c), recv.at[members + me, :, pl.ds(a, c)],
                     send_b, recv_a.at[k], mate, (pt, pj)).start()
            to_plane(one, True)
        for k in order[direct:]:
            push(k)
        for i, k in enumerate(order[direct:]):
            a, c = chunks[k]
            if i == min(RAW_SENT, last - direct):
                send_raw(beyond, members + me)
            settle(recv.at[pl.ds(0, members), :, pl.ds(a, c)], recv_a.at[k])
            copy(recv.at[pl.ds(0, members), :, pl.ds(a, c)], recv.at[pl.ds(members, members), :, pl.ds(a, c)],
                 send_b, recv_a.at[k], mate, (t, j)).start()
        settle(far.at[pl.ds(0, members)], send_r)
        settle(recv.at[pl.ds(0, members)], send_b)
        settle(recv.at[pl.ds(0, members - 1), :, pl.ds(chunks[direct][0], mine - chunks[direct][0])], send_a)
        settle(recv.at[pl.ds(0, members)], recv_o)


def solution(mesh):
    nt, ns = mesh.shape["tm"], mesh.shape["space"]

    def shards(thermal_field, seasonal_bucket, season_of_record):
        rows, cells = thermal_field.shape
        members, mine, e, swapped, raws = plan(nt, ns, cells)
        days = rows * nt * ns
        sems = pltpu.SemaphoreType.DMA
        per_chunk, per_swap = sems((len(swapped) + len(raws),)), sems((len(swapped),))
        vmem = functools.partial(pltpu.VMEM, dtype=jnp.float32)
        return pl.pallas_call(
            functools.partial(kernel, nt, ns),
            out_shape=jax.ShapeDtypeStruct((rows, cells), jnp.float32),
            in_specs=[pl.BlockSpec(memory_space=pltpu.HBM)] * 3,
            out_specs=pl.BlockSpec(memory_space=pltpu.VMEM),
            scratch_shapes=[
                pltpu.VMEM((2, 1, days), jnp.int32),
                vmem((rows, cells)),
                vmem((2 * members, rows, mine)),
                vmem((GROUPS, mine - e)),
                vmem((GROUPS, mine - e)),
                vmem((2 * members, rows, mine)),
                vmem((2 * members, rows, e)),
                sems, sems((2,)),
                sems, per_chunk, sems, sems, per_swap, sems, sems,
                sems, sems,
            ],
            compiler_params=pltpu.CompilerParams(
                collective_id=0, has_side_effects=True, vmem_limit_bytes=30 * 2**20),
            name="anomaly",
        )(*(pltpu.with_memory_space_constraint(a, pltpu.HBM) for a in (
            thermal_field, seasonal_bucket.reshape(1, -1), season_of_record.reshape(1, -1))))

    placed = (P(("tm", "space"), None), P(), P())
    return jax.shard_map(
        shards, mesh=mesh, in_specs=placed, out_specs=P(("tm", "space"), None), check_vma=False
    )
```

```python
import functools

import jax
import jax.numpy as jnp
from jax import lax
from jax.experimental import pallas as pl
from jax.experimental.pallas import tpu as pltpu
from jax.sharding import PartitionSpec as P

GROUPS = 46
BASE_YEARS = 6
PAIR = 2
PLANES = 4
UNIT = 128
RAW = 8
SIZES = (2, 3, 3, 3, 3, 3, 3, 3, 3, 3, 3, 3, 2, 1)
PIECES = 4
DIRECT = 2
LAG = 3
RAW_SENT = 0
RAW_FROM = 5
RAW_EVERY = 2
MESH = pl.DeviceIdType.MESH


def exact_dot(mask, x):
    high = x.astype(jnp.bfloat16)
    rest = x - high.astype(jnp.float32)
    middle = rest.astype(jnp.bfloat16)
    low = (rest - middle.astype(jnp.float32)).astype(jnp.bfloat16)
    total = jnp.dot(mask, low, preferred_element_type=jnp.float32)
    total += jnp.dot(mask, middle, preferred_element_type=jnp.float32)
    return total + jnp.dot(mask, high, preferred_element_type=jnp.float32)


def cuts(start, units, weights):
    total, edges = sum(weights), [0]
    for i in range(len(weights)):
        edge = units * sum(weights[:i + 1]) // total
        if edge > edges[-1]:
            edges.append(edge)
    return [(start + a * UNIT, (b - a) * UNIT) for a, b in zip(edges, edges[1:])]


def plan(nt, ns, cells):
    members = nt * (ns // PLANES)
    units = cells // members // UNIT
    raw = max(units * RAW // 48, 1)
    swapped = cuts(0, units - raw, SIZES)
    return members, units * UNIT, raw * UNIT, swapped, cuts((units - raw) * UNIT, raw, (1,) * PIECES)


def kernel(nt, ns, x_hbm, bucket_hbm, season_hbm, out_ref, calendar, xv, recv, sums, other, y, far,
           load_sem, date_sem, send_a, recv_a, send_b, send_s, recv_s, send_o, recv_o,
           send_r, recv_r):
    rows, cells = x_hbm.shape
    w = ns // PLANES
    members, mine, e, swapped, raws = plan(nt, ns, cells)
    chunks = swapped + raws
    last = len(swapped) - 1
    order = []
    for k in range(len(swapped)):
        order.append(k)
        order += [len(swapped) + i for i in range(len(raws))
                  if min(RAW_FROM + i * RAW_EVERY, last) == k]
    direct = min(DIRECT, len(swapped) - 1)
    days = rows * nt * ns
    t, s = lax.axis_index("tm"), lax.axis_index("space")
    q = s // w
    j = s - q * w
    me = t * w + j
    mate = q + 1 - 2 * lax.rem(q, 2)
    across = 3 - q
    beyond = 3 - mate
    is_mid = (q == 1) | (q == 2)
    is_outer = jnp.logical_not(is_mid)
    mine_at = pl.multiple_of(me * mine, UNIT)

    def copy(src, dst, send, recv_sem, plane, place):
        pt, pj = place
        return pltpu.make_async_remote_copy(
            src_ref=src, dst_ref=dst, send_sem=send, recv_sem=recv_sem,
            device_id=(pt, plane * w + pj), device_id_type=MESH)

    def settle(ref, sem):
        pltpu.make_async_copy(ref, ref, sem).wait()

    def to_plane(body, own=False):
        for dj in range(w):
            for dt in range(nt):
                if dt == dj == 0 and not own:
                    continue
                pt, pj = lax.rem(t + dt, nt), lax.rem(j + dj, w)
                body(pt, pj, pt * w + pj)

    load = pltpu.make_async_copy(x_hbm, xv, load_sem)
    load.start()
    barrier = pltpu.get_barrier_semaphore()

    def greet(plane, own):
        def one(pt, pj, p):
            pl.semaphore_signal(barrier, inc=1, device_id=(pt, plane * w + pj), device_id_type=MESH)
        to_plane(one, own)

    greet(q, False)

    @pl.when(is_mid)
    def _():
        for plane in (across, mate, beyond):
            greet(plane, True)

    dates = [pltpu.make_async_copy(ref, calendar.at[i], date_sem.at[i])
             for i, ref in enumerate((bucket_hbm, season_hbm))]

    def keep(k):
        a, c = chunks[k]
        pltpu.make_async_copy(x_hbm.at[:, pl.ds(pl.multiple_of(mine_at + a, UNIT), c)],
                              recv.at[me, :, pl.ds(a, c)], recv_a.at[k]).start()

    for k in order[direct:]:
        keep(k)

    def part(p, a, c):
        return xv.at[:, pl.ds(pl.multiple_of(p * mine + a, UNIT), c)]

    def push(k):
        a, c = chunks[k]

        def one(pt, pj, p):
            copy(part(p, a, c), recv.at[me, :, pl.ds(a, c)], send_a, recv_a.at[k], q, (pt, pj)).start()
        to_plane(one)

    def send_raw(plane, slot):
        def one(pt, pj, p):
            copy(part(p, mine - e, e), far.at[slot], send_r, recv_r, plane, (pt, pj)).start()
        to_plane(one, True)

    @pl.when(is_mid)
    def _():
        for k in range(direct):
            keep(k)
        for date in dates:
            date.start()
        pl.semaphore_wait(barrier, 2 * members - 1)
        load.wait()
        push(0)
        send_raw(across, me)
        for k in order[1:]:
            push(k)
        for date in dates:
            date.wait()

        bucket, season = calendar[0], calendar[1]
        key = jnp.where(season < BASE_YEARS, bucket, -1)
        padded = GROUPS
        here = 2 * members * rows

        def half(first, second):
            order = lax.broadcasted_iota(jnp.int32, (here, days), 0)
            plane = jnp.where(order < members * rows, first, second)
            p = lax.rem(order, members * rows) // rows
            day = ((p // w) * ns + plane * w + lax.rem(p, w)) * rows + lax.rem(order, rows)
            pick = day == lax.broadcasted_iota(jnp.int32, (here, days), 1)
            return lambda row: jnp.sum(jnp.where(pick, row, 0), axis=1, keepdims=True)

        def baseline(of_half):
            key_row = jnp.broadcast_to(of_half(key), (here, here)).T[:1]
            group = lax.broadcasted_iota(jnp.int32, (padded, here), 0)
            return jnp.where(group == key_row, 1.0, 0.0).astype(jnp.bfloat16)

        ours = half(q, mate)
        member = ours(bucket) == lax.broadcasted_iota(jnp.int32, (here, padded), 1)
        member = jnp.where(member, 1.0, 0.0).astype(jnp.bfloat16)
        of_ours, of_theirs = baseline(ours), baseline(half(across, beyond))
        counted = lax.broadcasted_iota(jnp.int32, (padded, days), 0) == key
        counts = jnp.sum(jnp.where(counted, 1.0, 0.0), axis=1, keepdims=True)
        inverse = 1.0 / jnp.maximum(counts, 1.0)

        def total(k):
            a, c = chunks[k]
            settle(recv.at[:, :, pl.ds(a, c)], recv_a.at[k])
            return exact_dot(of_ours, recv[:, :, pl.ds(a, c)].reshape(here, c))

        def swap(k):
            a, c = chunks[k]
            return copy(sums.at[:, :, pl.ds(a, c)], other.at[:, :, pl.ds(a, c)], send_s, recv_s.at[k], across, (t, j))

        def back(k, both):
            a, c = chunks[k]
            cols = pl.ds(a, c)
            at = pl.ds(pl.multiple_of(mine_at + a, UNIT), c)
            x = recv[:, :, cols].reshape(here, c)
            y[:, :, cols] = (x - exact_dot(member, both * inverse)).reshape(2 * members, rows, c)

            for p in range(members):
                copy(y.at[members + p, :, cols], out_ref.at[:, at], send_o, recv_o, mate, (p // w, p % w)).start()

            def near(pt, pj, p):
                copy(y.at[p, :, cols], out_ref.at[:, at], send_o, recv_o, q, (pt, pj)).start()
            to_plane(near)
            out_ref[:, at] = y[me, :, cols]

        def finish(k):
            a, c = chunks[k]
            swap(k).wait_recv()
            both = sums[:, :, pl.ds(a, c)] + other[:, :, pl.ds(a, c)]
            back(k, both.reshape(GROUPS, c))

        def finish_raw(k):
            a, c = chunks[k]
            if k == len(swapped):
                settle(far, recv_r)
            theirs = far[:, :, pl.ds(a - (mine - e), c)].reshape(here, c)
            back(k, total(k) + exact_dot(of_theirs, theirs))

        for k in order:
            if k > last:
                finish_raw(k)
                continue
            a, c = chunks[k]
            sums[:, :, pl.ds(a, c)] = total(k).reshape(GROUPS // PAIR, PAIR, c)
            swap(k).start()
            if k >= LAG:
                finish(k - LAG)
        for k in range(max(len(swapped) - LAG, 0), len(swapped)):
            finish(k)

        settle(sums, send_s)
        settle(far.at[pl.ds(0, members)], send_r)
        settle(y.at[pl.ds(0, 2 * members - 1)], send_o)
        settle(recv.at[pl.ds(0, members - 1)], recv_o)
        settle(recv.at[pl.ds(0, members - 1)], send_a)

    @pl.when(is_outer)
    def _():
        pl.semaphore_wait(barrier, 3 * members - 1)
        load.wait()
        for k, (a, c) in enumerate(chunks[:direct]):
            def one(pt, pj, p):
                copy(part(p, a, c), recv.at[members + me, :, pl.ds(a, c)],
                     send_b, recv_a.at[k], mate, (pt, pj)).start()
            to_plane(one, True)
        for k in order[direct:]:
            push(k)
        for i, k in enumerate(order[direct:]):
            a, c = chunks[k]
            if i == min(RAW_SENT, last - direct):
                send_raw(beyond, members + me)
            settle(recv.at[pl.ds(0, members), :, pl.ds(a, c)], recv_a.at[k])
            copy(recv.at[pl.ds(0, members), :, pl.ds(a, c)], recv.at[pl.ds(members, members), :, pl.ds(a, c)],
                 send_b, recv_a.at[k], mate, (t, j)).start()
        settle(far.at[pl.ds(0, members)], send_r)
        settle(recv.at[pl.ds(0, members)], send_b)
        settle(recv.at[pl.ds(0, members - 1), :, pl.ds(chunks[direct][0], mine - chunks[direct][0])], send_a)
        settle(recv.at[pl.ds(0, members)], recv_o)


def solution(mesh):
    nt, ns = mesh.shape["tm"], mesh.shape["space"]

    def shards(thermal_field, seasonal_bucket, season_of_record):
        rows, cells = thermal_field.shape
        members, mine, e, swapped, raws = plan(nt, ns, cells)
        days = rows * nt * ns
        sems = pltpu.SemaphoreType.DMA
        per_chunk, per_swap = sems((len(swapped) + len(raws),)), sems((len(swapped),))
        vmem = functools.partial(pltpu.VMEM, dtype=jnp.float32)
        return pl.pallas_call(
            functools.partial(kernel, nt, ns),
            out_shape=jax.ShapeDtypeStruct((rows, cells), jnp.float32),
            in_specs=[pl.BlockSpec(memory_space=pltpu.HBM)] * 3,
            out_specs=pl.BlockSpec(memory_space=pltpu.VMEM),
            scratch_shapes=[
                pltpu.VMEM((2, 1, days), jnp.int32),
                vmem((rows, cells)),
                vmem((2 * members, rows, mine)),
                vmem((GROUPS // PAIR, PAIR, mine - e)),
                vmem((GROUPS // PAIR, PAIR, mine - e)),
                vmem((2 * members, rows, mine)),
                vmem((2 * members, rows, e)),
                sems, sems((2,)),
                sems, per_chunk, sems, sems, per_swap, sems, sems,
                sems, sems,
            ],
            compiler_params=pltpu.CompilerParams(
                collective_id=0, has_side_effects=True, vmem_limit_bytes=30 * 2**20),
            name="anomaly",
        )(*(pltpu.with_memory_space_constraint(a, pltpu.HBM) for a in (
            thermal_field, seasonal_bucket.reshape(1, -1), season_of_record.reshape(1, -1))))

    placed = (P(("tm", "space"), None), P(), P())
    return jax.shard_map(
        shards, mesh=mesh, in_specs=placed, out_specs=P(("tm", "space"), None), check_vma=False
    )
```

```python
import functools

import jax
import jax.numpy as jnp
from jax import lax
from jax.experimental import pallas as pl
from jax.experimental.pallas import tpu as pltpu
from jax.sharding import PartitionSpec as P

GROUPS = 46
BASE_YEARS = 6
PAIR = 2
PLANES = 4
UNIT = 128
RAW = 8
SIZES = (2, 3, 3, 3, 3, 3, 3, 3, 3, 3, 3, 3, 2, 1)
PIECES = 4
DIRECT = 2
LAG = 3
RAW_SENT = 0
RAW_FROM = 5
RAW_EVERY = 2
MESH = pl.DeviceIdType.MESH


def exact_dot(mask, x):
    high = x.astype(jnp.bfloat16)
    rest = x - high.astype(jnp.float32)
    middle = rest.astype(jnp.bfloat16)
    low = (rest - middle.astype(jnp.float32)).astype(jnp.bfloat16)
    total = jnp.dot(mask, low, preferred_element_type=jnp.float32)
    total += jnp.dot(mask, middle, preferred_element_type=jnp.float32)
    return total + jnp.dot(mask, high, preferred_element_type=jnp.float32)


def cuts(start, units, weights):
    total, edges = sum(weights), [0]
    for i in range(len(weights)):
        edge = units * sum(weights[:i + 1]) // total
        if edge > edges[-1]:
            edges.append(edge)
    return [(start + a * UNIT, (b - a) * UNIT) for a, b in zip(edges, edges[1:])]


def plan(nt, ns, cells):
    members = nt * (ns // PLANES)
    units = cells // members // UNIT
    raw = max(units * RAW // 48, 1)
    swapped = cuts(0, units - raw, SIZES)
    return members, units * UNIT, raw * UNIT, swapped, cuts((units - raw) * UNIT, raw, (1,) * PIECES)


def kernel(nt, ns, x_hbm, bucket_hbm, season_hbm, out_ref, calendar, xv, recv, y, far,
           load_sem, date_sem, send_a, recv_a, send_b, send_s, recv_s, send_o, recv_o,
           send_r, recv_r, *pairs):
    rows, cells = x_hbm.shape
    w = ns // PLANES
    members, mine, e, swapped, raws = plan(nt, ns, cells)
    chunks = swapped + raws
    sums, other = pairs[:len(swapped)], pairs[len(swapped):]
    last = len(swapped) - 1
    order = []
    for k in range(len(swapped)):
        order.append(k)
        order += [len(swapped) + i for i in range(len(raws))
                  if min(RAW_FROM + i * RAW_EVERY, last) == k]
    direct = min(DIRECT, len(swapped) - 1)
    days = rows * nt * ns
    t, s = lax.axis_index("tm"), lax.axis_index("space")
    q = s // w
    j = s - q * w
    me = t * w + j
    mate = q + 1 - 2 * lax.rem(q, 2)
    across = 3 - q
    beyond = 3 - mate
    is_mid = (q == 1) | (q == 2)
    is_outer = jnp.logical_not(is_mid)
    mine_at = pl.multiple_of(me * mine, UNIT)

    def copy(src, dst, send, recv_sem, plane, place):
        pt, pj = place
        return pltpu.make_async_remote_copy(
            src_ref=src, dst_ref=dst, send_sem=send, recv_sem=recv_sem,
            device_id=(pt, plane * w + pj), device_id_type=MESH)

    def settle(ref, sem):
        pltpu.make_async_copy(ref, ref, sem).wait()

    def to_plane(body, own=False):
        for dj in range(w):
            for dt in range(nt):
                if dt == dj == 0 and not own:
                    continue
                pt, pj = lax.rem(t + dt, nt), lax.rem(j + dj, w)
                body(pt, pj, pt * w + pj)

    load = pltpu.make_async_copy(x_hbm, xv, load_sem)
    load.start()
    barrier = pltpu.get_barrier_semaphore()

    def greet(plane, own):
        def one(pt, pj, p):
            pl.semaphore_signal(barrier, inc=1, device_id=(pt, plane * w + pj), device_id_type=MESH)
        to_plane(one, own)

    greet(q, False)

    @pl.when(is_mid)
    def _():
        for plane in (across, mate, beyond):
            greet(plane, True)

    dates = [pltpu.make_async_copy(ref, calendar.at[i], date_sem.at[i])
             for i, ref in enumerate((bucket_hbm, season_hbm))]

    def keep(k):
        a, c = chunks[k]
        pltpu.make_async_copy(x_hbm.at[:, pl.ds(pl.multiple_of(mine_at + a, UNIT), c)],
                              recv.at[me, :, pl.ds(a, c)], recv_a.at[k]).start()

    for k in order[direct:]:
        keep(k)

    def part(p, a, c):
        return xv.at[:, pl.ds(pl.multiple_of(p * mine + a, UNIT), c)]

    def push(k):
        a, c = chunks[k]

        def one(pt, pj, p):
            copy(part(p, a, c), recv.at[me, :, pl.ds(a, c)], send_a, recv_a.at[k], q, (pt, pj)).start()
        to_plane(one)

    def send_raw(plane, slot):
        def one(pt, pj, p):
            copy(part(p, mine - e, e), far.at[slot], send_r, recv_r, plane, (pt, pj)).start()
        to_plane(one, True)

    @pl.when(is_mid)
    def _():
        for k in range(direct):
            keep(k)
        for date in dates:
            date.start()
        pl.semaphore_wait(barrier, 2 * members - 1)
        load.wait()
        send_raw(across, me)
        push(0)
        for k in order[1:]:
            push(k)
        for date in dates:
            date.wait()

        bucket, season = calendar[0], calendar[1]
        key = jnp.where(season < BASE_YEARS, bucket, -1)
        padded = GROUPS
        here = 2 * members * rows

        def half(first, second):
            order = lax.broadcasted_iota(jnp.int32, (here, days), 0)
            plane = jnp.where(order < members * rows, first, second)
            p = lax.rem(order, members * rows) // rows
            day = ((p // w) * ns + plane * w + lax.rem(p, w)) * rows + lax.rem(order, rows)
            pick = day == lax.broadcasted_iota(jnp.int32, (here, days), 1)
            return lambda row: jnp.sum(jnp.where(pick, row, 0), axis=1, keepdims=True)

        def baseline(of_half):
            key_row = jnp.broadcast_to(of_half(key), (here, here)).T[:1]
            group = lax.broadcasted_iota(jnp.int32, (padded, here), 0)
            return jnp.where(group == key_row, 1.0, 0.0).astype(jnp.bfloat16)

        ours = half(q, mate)
        member = ours(bucket) == lax.broadcasted_iota(jnp.int32, (here, padded), 1)
        member = jnp.where(member, 1.0, 0.0).astype(jnp.bfloat16)
        of_ours, of_theirs = baseline(ours), baseline(half(across, beyond))
        counted = lax.broadcasted_iota(jnp.int32, (padded, days), 0) == key
        counts = jnp.sum(jnp.where(counted, 1.0, 0.0), axis=1, keepdims=True)
        inverse = 1.0 / jnp.maximum(counts, 1.0)

        def total(k):
            a, c = chunks[k]
            settle(recv.at[:, :, pl.ds(a, c)], recv_a.at[k])
            return exact_dot(of_ours, recv[:, :, pl.ds(a, c)].reshape(here, c))

        def swap(k):
            return copy(sums[k], other[k], send_s, recv_s.at[k], across, (t, j))

        def back(k, both):
            a, c = chunks[k]
            cols = pl.ds(a, c)
            at = pl.ds(pl.multiple_of(mine_at + a, UNIT), c)
            x = recv[:, :, cols].reshape(here, c)
            y[:, :, cols] = (x - exact_dot(member, both * inverse)).reshape(2 * members, rows, c)

            for p in range(members):
                copy(y.at[members + p, :, cols], out_ref.at[:, at], send_o, recv_o, mate, (p // w, p % w)).start()

            def near(pt, pj, p):
                copy(y.at[p, :, cols], out_ref.at[:, at], send_o, recv_o, q, (pt, pj)).start()
            to_plane(near)
            out_ref[:, at] = y[me, :, cols]

        def finish(k):
            swap(k).wait_recv()
            back(k, (sums[k][...] + other[k][...]).reshape(GROUPS, chunks[k][1]))

        def finish_raw(k):
            a, c = chunks[k]
            if k == len(swapped):
                settle(far, recv_r)
            theirs = far[:, :, pl.ds(a - (mine - e), c)].reshape(here, c)
            back(k, total(k) + exact_dot(of_theirs, theirs))

        for k in order:
            if k > last:
                finish_raw(k)
                continue
            sums[k][...] = total(k).reshape(sums[k].shape)
            swap(k).start()
            if k >= LAG:
                finish(k - LAG)
        for k in range(max(len(swapped) - LAG, 0), len(swapped)):
            finish(k)

        for part_sums in sums:
            settle(part_sums, send_s)
        settle(far.at[pl.ds(0, members)], send_r)
        settle(y.at[pl.ds(0, 2 * members - 1)], send_o)
        settle(recv.at[pl.ds(0, members - 1)], recv_o)
        settle(recv.at[pl.ds(0, members - 1)], send_a)

    @pl.when(is_outer)
    def _():
        pl.semaphore_wait(barrier, 3 * members - 1)
        load.wait()
        for k, (a, c) in enumerate(chunks[:direct]):
            def one(pt, pj, p):
                copy(part(p, a, c), recv.at[members + me, :, pl.ds(a, c)],
                     send_b, recv_a.at[k], mate, (pt, pj)).start()
            to_plane(one, True)
        for k in order[direct:]:
            push(k)
        for i, k in enumerate(order[direct:]):
            a, c = chunks[k]
            if i == min(RAW_SENT, last - direct):
                send_raw(beyond, members + me)
            settle(recv.at[pl.ds(0, members), :, pl.ds(a, c)], recv_a.at[k])
            copy(recv.at[pl.ds(0, members), :, pl.ds(a, c)], recv.at[pl.ds(members, members), :, pl.ds(a, c)],
                 send_b, recv_a.at[k], mate, (t, j)).start()
        settle(far.at[pl.ds(0, members)], send_r)
        settle(recv.at[pl.ds(0, members)], send_b)
        settle(recv.at[pl.ds(0, members - 1), :, pl.ds(chunks[direct][0], mine - chunks[direct][0])], send_a)
        settle(recv.at[pl.ds(0, members)], recv_o)


def solution(mesh):
    nt, ns = mesh.shape["tm"], mesh.shape["space"]

    def shards(thermal_field, seasonal_bucket, season_of_record):
        rows, cells = thermal_field.shape
        members, mine, e, swapped, raws = plan(nt, ns, cells)
        days = rows * nt * ns
        sems = pltpu.SemaphoreType.DMA
        per_chunk, per_swap = sems((len(swapped) + len(raws),)), sems((len(swapped),))
        vmem = functools.partial(pltpu.VMEM, dtype=jnp.float32)
        return pl.pallas_call(
            functools.partial(kernel, nt, ns),
            out_shape=jax.ShapeDtypeStruct((rows, cells), jnp.float32),
            in_specs=[pl.BlockSpec(memory_space=pltpu.HBM)] * 3,
            out_specs=pl.BlockSpec(memory_space=pltpu.VMEM),
            scratch_shapes=[
                pltpu.VMEM((2, 1, days), jnp.int32),
                vmem((rows, cells)),
                vmem((2 * members, rows, mine)),
                vmem((2 * members, rows, mine)),
                vmem((2 * members, rows, e)),
                sems, sems((2,)),
                sems, per_chunk, sems, sems, per_swap, sems, sems,
                sems, sems,
                *[vmem((GROUPS // PAIR, PAIR, c)) for _, c in swapped * 2],
            ],
            compiler_params=pltpu.CompilerParams(
                collective_id=0, has_side_effects=True, vmem_limit_bytes=30 * 2**20),
            name="anomaly",
        )(*(pltpu.with_memory_space_constraint(a, pltpu.HBM) for a in (
            thermal_field, seasonal_bucket.reshape(1, -1), season_of_record.reshape(1, -1))))

    placed = (P(("tm", "space"), None), P(), P())
    return jax.shard_map(
        shards, mesh=mesh, in_specs=placed, out_specs=P(("tm", "space"), None), check_vma=False
    )
```
